32 devices in a mesh: vocab: 8 (over z, x), tok: 4 (over y, core).
Axes of the slice: x: 2, y: 2, z: 4, core: 2. Of those that a mesh axis runs over, the one named last changes fastest.
Arguments:
- hidden: bfloat16 [768, 7168], P('tok', 'vocab'), may hold values from -21 to 21
- head_weight: bfloat16 [7168, 8192], P('tok', 'vocab'), may hold values from -0.12695312 to 0.12695312
- targets: int32 [768], P('tok'), may hold values from 0 to 6143
- vocab_mask: int32 [8192], P('vocab'), may hold values from 0 to 1, as said below
- token_grad: float32 [768], P('tok'), may hold values from 16 to 160
Outputs:
- hidden_grad: bfloat16 [768, 7168], P('tok', 'vocab')
- token_loss: float32 [768], P('tok')
The draws below stay inside these ranges and needn't reach their ends.
Inputs may be any that keep to these rules, and one draw needn't show every extreme that they name: vocab_mask is 1 on the columns below some cut and 0 from it on, with between 1 and 2048 zeros.
All inputs are finite; a program needn't handle non-finite values.
Results may differ from the reference program's by a relative error of at most 0.0051.
Values may be sent and summed in bfloat16 or wider, within the bound.
A program may use at most 64 MiB of HBM per device.

```python
import math
import jax
import jax.numpy as jnp
from jax import lax

D = 7168
V = 8192
TOKENS = 768


def draw_head_weight(key, part):
    weights = jnp.clip(jax.random.normal(jax.random.fold_in(key, 11), (D, V), jnp.float32), -6.0, 6.0) * D ** (-0.5)
    return weights.astype(jnp.bfloat16)


def draw_hidden(key, part):
    values = 3.0 * jnp.clip(jax.random.normal(jax.random.fold_in(key, 23), (TOKENS, D), jnp.float32), -6.0, 6.0)
    return values.astype(jnp.bfloat16)


def draw_vocab_mask(key, part):
    padding = jax.random.randint(jax.random.fold_in(key, 31), (), 1, V // 4 + 1)
    return (jnp.arange(V, dtype=jnp.int32) < V - padding).astype(jnp.int32)


def with_ends(values, own_key, low, high):
    spot = [jax.random.randint(jax.random.fold_in(own_key, axis), (), 0, length) for axis, length in enumerate(values.shape)]
    widest = values.shape.index(max(values.shape))
    next_to = spot[:widest] + [(spot[widest] + 1) % values.shape[widest]] + spot[widest + 1:]
    return values.at[tuple(spot)].set(low).at[tuple(next_to)].set(high)


def steps_of(stream_key, dims, shards, least, top_value):
    def one(position, shards_of):
        heights = jax.random.uniform(jax.random.fold_in(jax.random.fold_in(stream_key, 6), position), (shards_of,), jnp.float32, least / len(shards), top_value / len(shards))
        return jnp.repeat(jnp.exp(heights), dims[position] // shards_of).reshape((-1,) + (1,) * (len(dims) - position - 1))

    factor_of = one(*shards[0])
    for cut in shards[1:]:
        factor_of = factor_of * one(*cut)
    return factor_of


def setup_inputs(seed: int = 0) -> dict:
    keys = jax.random.split(jax.random.key(seed), 6)
    hidden = draw_hidden(jax.random.fold_in(keys[5], 71), 0)
    head_weight = draw_head_weight(jax.random.fold_in(keys[5], 71), 0)
    targets = with_ends(jax.random.randint(keys[2], (TOKENS,), 0, 3 * V // 4), jax.random.fold_in(keys[2], 1), 0, (3 * V // 4) - 1).astype(jnp.int32)
    vocab_mask = draw_vocab_mask(jax.random.fold_in(keys[5], 71), 0)
    token_grad = jnp.clip(jnp.exp(math.log(160.0) - 2.3025851 * jax.random.uniform(keys[4], (TOKENS,), jnp.float32) ** steps_of(keys[4], (TOKENS,), ((0, 4),), -0.2, 0.2)), 16.0, 160.0)
    return dict(hidden=hidden, head_weight=head_weight, targets=targets, vocab_mask=vocab_mask, token_grad=token_grad)


def reference(hidden, head_weight, targets, vocab_mask, token_grad):
    logits = jnp.dot(hidden, head_weight, preferred_element_type=jnp.float32)
    live_mask = vocab_mask[None, :] == 1
    masked = jnp.where(live_mask, logits, jnp.float32(-1e30))
    row_max = jnp.max(masked, axis=1)
    denominator = jnp.sum(jnp.exp(masked - row_max[:, None]), axis=1)
    columns = jnp.arange(V, dtype=jnp.int32)
    onehot = columns[None, :] == targets[:, None].astype(jnp.int32)
    target_logit = jnp.sum(jnp.where(onehot, logits, jnp.float32(0.0)), axis=1)
    log_norm = row_max + jnp.log(denominator)
    token_loss = log_norm - target_logit
    probabilities = jnp.exp(masked - log_norm[:, None])
    logit_grad = (token_grad[:, None] * (probabilities - onehot.astype(jnp.float32))).astype(jnp.bfloat16)
    hidden_grad = lax.dot_general(logit_grad, head_weight, (((1,), (1,)), ((), ())), preferred_element_type=jnp.float32)
    return hidden_grad.astype(jnp.bfloat16), token_loss
```

```python
import jax
import jax.numpy as jnp
from jax import lax
from jax.sharding import PartitionSpec as P


def make_on_device(vocab_size, tok_size):
    share = vocab_size // tok_size
    moves = [
        (b * tok_size + a, (a * share + b % share) * tok_size + b // share)
        for a in range(tok_size)
        for b in range(vocab_size)
    ]
    back = [(there, here) for here, there in moves]

    def on_device(hidden, head_weight, targets, vocab_mask, token_grad):
        rows, feats = hidden.shape
        block_width = head_weight.shape[1]
        moved = lax.ppermute(hidden, ("vocab", "tok"), moves)
        pieces = lax.all_gather(moved, "vocab")
        gathered = (
            pieces.reshape(tok_size, share, rows, feats)
            .transpose(0, 2, 1, 3)
            .reshape(tok_size * rows, share * feats)
        )
        partial_logits = jnp.dot(gathered, head_weight, preferred_element_type=jnp.float32)
        logits = lax.psum_scatter(partial_logits, "tok", scatter_dimension=0, tiled=True)
        first_column = lax.axis_index("vocab") * block_width
        masked = jnp.where(vocab_mask[None, :] == 1, logits, jnp.float32(-1e30))
        local_max = jnp.max(masked, axis=1)
        columns = first_column + jnp.arange(block_width, dtype=jnp.int32)
        onehot = columns[None, :] == targets[:, None]
        local_target = jnp.sum(jnp.where(onehot, logits, jnp.float32(0.0)), axis=1)
        weights = jnp.exp(masked - local_max[:, None])
        local_sum = jnp.sum(weights, axis=1)
        stats = lax.all_gather(jnp.stack([local_max, local_sum, local_target]), "vocab")
        row_max = jnp.max(stats[:, 0], axis=0)
        denominator = jnp.sum(stats[:, 1] * jnp.exp(stats[:, 0] - row_max[None]), axis=0)
        target_logit = jnp.sum(stats[:, 2], axis=0)
        log_norm = row_max + jnp.log(denominator)
        token_loss = log_norm - target_logit
        probabilities = jnp.exp(masked - log_norm[:, None])
        logit_grad = (
            token_grad[:, None] * (probabilities - onehot.astype(jnp.float32))
        ).astype(jnp.bfloat16)
        all_grads = lax.all_gather(logit_grad, "tok", axis=0, tiled=True)
        partial_value = lax.dot_general(
            all_grads,
            head_weight,
            (((1,), (1,)), ((), ())),
            preferred_element_type=jnp.float32,
        )
        blocks = (
            partial_value.reshape(tok_size, rows, share, feats)
            .transpose(0, 2, 1, 3)
            .reshape(vocab_size, rows, feats)
        )
        summed = lax.psum_scatter(blocks, "vocab", scatter_dimension=0, tiled=False)
        hidden_grad = lax.ppermute(summed.astype(jnp.bfloat16), ("vocab", "tok"), back)
        return (hidden_grad, token_loss)

    return on_device


def solution(mesh):
    placed = (P("tok", "vocab"), P("tok", "vocab"), P("tok"), P("vocab"), P("tok"))
    return jax.shard_map(
        make_on_device(mesh.shape["vocab"], mesh.shape["tok"]),
        mesh=mesh,
        in_specs=placed,
        out_specs=(P("tok", "vocab"), P("tok")),
        check_vma=False,
    )
```

```python
import jax
import jax.numpy as jnp
from jax import lax
from jax.experimental import pallas as pl
from jax.experimental.pallas import tpu as pltpu
from jax.sharding import PartitionSpec as P


def make_on_device(vocab_size, tok_size):
    share = vocab_size // tok_size
    moves = [
        (b * tok_size + a, (a * share + b % share) * tok_size + b // share)
        for a in range(tok_size)
        for b in range(vocab_size)
    ]
    back = [(there, here) for here, there in moves]

    def on_device(hidden, head_weight, targets, vocab_mask, token_grad):
        rows, feats = hidden.shape
        block_width = head_weight.shape[1]
        moved = lax.ppermute(hidden, ("vocab", "tok"), moves)
        pieces = lax.all_gather(moved, "vocab")
        gathered = (
            pieces.reshape(tok_size, share, rows, feats)
            .transpose(0, 2, 1, 3)
            .reshape(tok_size * rows, share * feats)
        )
        partial_logits = jnp.dot(gathered, head_weight, preferred_element_type=jnp.float32)
        logits = lax.psum_scatter(partial_logits, "tok", scatter_dimension=0, tiled=True)
        first_column = lax.axis_index("vocab") * block_width
        masked = jnp.where(vocab_mask[None, :] == 1, logits, jnp.float32(-1e30))
        local_max = jnp.max(masked, axis=1)
        columns = first_column + jnp.arange(block_width, dtype=jnp.int32)
        onehot = columns[None, :] == targets[:, None]
        local_target = jnp.sum(jnp.where(onehot, logits, jnp.float32(0.0)), axis=1)
        weights = jnp.exp(masked - local_max[:, None])
        local_sum = jnp.sum(weights, axis=1)
        stats = lax.all_gather(jnp.stack([local_max, local_sum, local_target]), "vocab")
        row_max = jnp.max(stats[:, 0], axis=0)
        denominator = jnp.sum(stats[:, 1] * jnp.exp(stats[:, 0] - row_max[None]), axis=0)
        target_logit = jnp.sum(stats[:, 2], axis=0)
        log_norm = row_max + jnp.log(denominator)
        token_loss = log_norm - target_logit
        probabilities = jnp.exp(masked - log_norm[:, None])
        logit_grad = (
            token_grad[:, None] * (probabilities - onehot.astype(jnp.float32))
        ).astype(jnp.bfloat16)
        all_grads = lax.all_gather(logit_grad, "tok", axis=0, tiled=True)
        partial_value = lax.dot_general(
            all_grads,
            head_weight,
            (((1,), (1,)), ((), ())),
            preferred_element_type=jnp.float32,
        )
        blocks = (
            partial_value.reshape(tok_size, rows, share, feats)
            .transpose(0, 2, 1, 3)
            .reshape(vocab_size, rows, feats)
        )
        summed = lax.psum_scatter(blocks, "vocab", scatter_dimension=0, tiled=False)
        hidden_grad = lax.ppermute(summed.astype(jnp.bfloat16), ("vocab", "tok"), back)
        return (hidden_grad, token_loss)

    return on_device


CHUNKS = 2
BF = jnp.bfloat16
F32 = jnp.float32


def kernel(
    depth,
    hidden_ref, weight_ref, targets_ref, mask_ref, grad_ref,
    out_ref, loss_ref,
    gath, hb, plog, pair_in, cross_in, cross_out, dl, stats_out, stats_in,
    term_out, term_in, up_in, down_in, up_out, down_out, far_out, far_in,
    load_sem, x_send, x_recv, zu_send, zu_recv, zd_send, zd_recv, t_send, t_recv,
    p_send, p_recv, c_send, c_recv, s_send, s_recv, g_send, g_recv,
    e_send, e_recv, eu_send, eu_recv, ed_send, ed_recv, f_send, f_recv,
):
    rows, feats = hidden_ref.shape
    part = rows // CHUNKS
    width = weight_ref.shape[1]
    me_v = lax.axis_index("vocab")
    me_t = lax.axis_index("tok")
    z, x = me_v // 2, me_v % 2
    y, c = me_t // 2, me_t % 2
    nv = 2 * depth

    def dev(v, t):
        return {"vocab": v, "tok": t}

    def tok_of(r):
        return ((y + r // 2) % 2) * 2 + (c + r % 2) % 2

    other_x = z * 2 + (1 - x)

    def rcopy(src, dst, ss, rs, v, t):
        return pltpu.make_async_remote_copy(
            src_ref=src, dst_ref=dst, send_sem=ss, recv_sem=rs,
            device_id=dev(v, t), device_id_type=pl.DeviceIdType.MESH,
        )

    def span(h):
        return pl.ds(h * part, part)

    loads = [
        pltpu.make_async_copy(hidden_ref.at[span(h)], gath.at[0, z, h], load_sem.at[h])
        for h in range(CHUNKS)
    ]
    for load in loads:
        load.start()

    barrier = pltpu.get_barrier_semaphore()
    for r in range(1, 4):
        pl.semaphore_signal(barrier, inc=1, device_id=dev(me_v, tok_of(r)), device_id_type=pl.DeviceIdType.MESH)
    for k in range(1, nv):
        pl.semaphore_signal(barrier, inc=1, device_id=dev((me_v + k) % nv, me_t), device_id_type=pl.DeviceIdType.MESH)
    pl.semaphore_wait(barrier, 3 + nv - 1)

    def x_copy(h):
        return rcopy(gath.at[0, z, h], gath.at[1, z, h], x_send.at[h], x_recv.at[h], other_x, me_t)

    def up_copy(q, zz, h):
        return rcopy(gath.at[q, zz, h], gath.at[q, zz, h], zu_send.at[q, zz, h], zu_recv.at[q, zz, h], me_v + 2, me_t)

    def down_copy(q, zz, h):
        return rcopy(gath.at[q, zz, h], gath.at[q, zz, h], zd_send.at[q, zz, h], zd_recv.at[q, zz, h], me_v - 2, me_t)

    def rel(zz):
        return 2 * ((zz // 2 + y) % 2) + (zz % 2 + c) % 2

    def t_copy(q, zz, h):
        r = rel(zz)
        return rcopy(gath.at[q, zz, h], hb.at[q, r, h], t_send.at[q, zz, h], t_recv.at[q, r, h], me_v, zz)

    def pass_on(q, zz, h):
        @pl.when(zz != me_t)
        def _():
            t_copy(q, zz, h).start()

    for h in range(CHUNKS):
        loads[h].wait()
        x_copy(h).start()
    for s in range(depth):
        for h in range(CHUNKS):
            for q in range(2):
                if s == 0:
                    if q == 1:
                        x_copy(h).wait_recv()

                    @pl.when(z < depth - 1)
                    def _():
                        up_copy(q, z, h).start()

                    @pl.when(z > 0)
                    def _():
                        down_copy(q, z, h).start()

                    pass_on(q, z, h)
                else:
                    @pl.when(z - s >= 0)
                    def _():
                        up_copy(q, z - s, h).wait_recv()

                        @pl.when(z < depth - 1)
                        def _():
                            up_copy(q, z - s, h).start()

                        pass_on(q, z - s, h)

                    @pl.when(z + s < depth)
                    def _():
                        down_copy(q, z + s, h).wait_recv()

                        @pl.when(z > 0)
                        def _():
                            down_copy(q, z + s, h).start()

                        pass_on(q, z + s, h)

    for q in range(2):
        for h in range(CHUNKS):
            hb[q, 0, h] = gath[q, me_t, h]

    def weight_rows(q):
        owner = (x + q) % 2
        return pl.ds(pl.multiple_of(owner * feats, 128), feats)

    tile = 256

    def logits_of(r0, nr):
        @pl.loop(0, width // tile)
        def _(j):
            cols = pl.ds(pl.multiple_of(j * tile, tile), tile)
            total = None
            for q in range(2):
                lhs = hb[q, pl.ds(r0, nr)].reshape(nr * rows, feats)
                term = jnp.dot(lhs, weight_ref[weight_rows(q), cols], preferred_element_type=F32)
                total = term if total is None else total + term
            plog[pl.ds(r0, nr), :, cols] = total.reshape(nr, rows, tile)

    def pair_copy(k):
        return rcopy(plog.at[1 + 2 * k], pair_in.at[k], p_send.at[k], p_recv.at[k], me_v, tok_of(1))

    def cross_copy():
        return rcopy(cross_out, cross_in, c_send.at[0], c_recv.at[0], me_v, tok_of(2))

    def await_rel(r):
        for q in range(2):
            for h in range(CHUNKS):
                rcopy(gath.at[q, 0, h], hb.at[q, r, h], t_send.at[q, 0, h], t_recv.at[q, r, h], me_v, tok_of(1)).wait_recv()

    await_rel(2)
    await_rel(3)
    logits_of(2, 2)
    pair_copy(1).start()
    await_rel(1)
    logits_of(0, 2)
    pair_copy(0).start()
    pair_copy(1).wait_recv()
    cross_out[...] = plog[2] + pair_in[1]
    cross_copy().start()
    pair_copy(0).wait_recv()
    plog[0] = plog[0] + pair_in[0]
    cross_copy().wait_recv()
    logits = plog[0] + cross_in[...]

    masked = jnp.where(mask_ref[...] == 1, logits, jnp.float32(-1e30))
    local_max = jnp.max(masked, axis=1, keepdims=True)
    columns = me_v * width + lax.broadcasted_iota(jnp.int32, (rows, width), 1)
    onehot = columns == targets_ref[...]
    local_target = jnp.sum(jnp.where(onehot, logits, 0.0), axis=1, keepdims=True)
    local_sum = jnp.sum(jnp.exp(masked - local_max), axis=1, keepdims=True)
    lanes = lax.broadcasted_iota(jnp.int32, (rows, 128), 1)
    packed = jnp.where(lanes == 0, local_max, jnp.where(lanes == 1, local_sum, local_target))
    tall = jnp.concatenate([packed, jnp.zeros((256 - rows, 128), F32)], axis=0)
    mine = jnp.transpose(tall)[0:8]
    stats_out[...] = mine
    stats_in[me_v] = mine
    plog[0] = masked

    def stat_copy(k):
        return rcopy(stats_out, stats_in.at[me_v], s_send.at[k], s_recv.at[me_v], (me_v + k) % nv, me_t)

    for k in range(1, nv):
        stat_copy(k).start()
    for k in range(1, nv):
        source = (me_v + nv - k) % nv
        rcopy(stats_out, stats_in.at[source], s_send.at[k], s_recv.at[source], source, me_t).wait_recv()
    row_max = stats_in[0][0:1]
    for v in range(1, nv):
        row_max = jnp.maximum(row_max, stats_in[v][0:1])
    denominator = jnp.zeros_like(row_max)
    target_logit = jnp.zeros_like(row_max)
    for v in range(nv):
        got = stats_in[v]
        denominator += got[1:2] * jnp.exp(got[0:1] - row_max)
        target_logit += got[2:3]
    log_norm = row_max + jnp.log(denominator)
    loss_ref[...] = jnp.broadcast_to(log_norm - target_logit, loss_ref.shape)
    column = jnp.transpose(jnp.broadcast_to(log_norm, (128, 256)))[0:rows, 0:1]
    probabilities = jnp.exp(plog[0] - column)
    dl[0] = (grad_ref[...] * (probabilities - onehot.astype(F32))).astype(BF)

    def grad_copy(i):
        if i == 0:
            return rcopy(dl.at[0], dl.at[2], g_send.at[0], g_recv.at[0], me_v, tok_of(2))
        if i == 1:
            return rcopy(dl.at[0], dl.at[1], g_send.at[1], g_recv.at[1], me_v, tok_of(1))
        return rcopy(dl.at[2], dl.at[3], g_send.at[2], g_recv.at[2], me_v, tok_of(1))

    grad_copy(0).start()
    grad_copy(1).start()

    def term_copy(q, r, h):
        return rcopy(
            term_out.at[q, r, h], term_in.at[q, me_t, h], e_send.at[q, r, h], e_recv.at[q, r, h], me_v, tok_of(r)
        )

    def terms_of(q, r0):
        lhs = dl[pl.ds(r0, 2)].reshape(2 * rows, width)
        value = lax.dot_general(
            lhs, weight_ref[weight_rows(q), :], (((1,), (1,)), ((), ())), preferred_element_type=F32
        ).astype(BF).reshape(2, CHUNKS, part, feats)
        for i in range(2):
            if r0 + i == 0:
                term_in[q, me_t] = value[0]
            else:
                term_out[q, r0 + i] = value[i]

    grad_copy(1).wait_recv()
    for q in (1, 0):
        terms_of(q, 0)
    grad_copy(0).wait_recv()
    grad_copy(2).start()
    grad_copy(2).wait_recv()
    for q in (1, 0):
        terms_of(q, 2)
        for h in range(CHUNKS):
            for r in (2, 3, 1):
                term_copy(q, r, h).start()

    def eu_copy(q, zz, h):
        return rcopy(up_out.at[q, zz, h], up_in.at[q, zz, h], eu_send.at[q, zz, h], eu_recv.at[q, zz, h], me_v + 2, me_t)

    def ed_copy(q, zz, h):
        return rcopy(down_out.at[q, zz, h], down_in.at[q, zz, h], ed_send.at[q, zz, h], ed_recv.at[q, zz, h], me_v - 2, me_t)

    def far_copy(h):
        return rcopy(far_out.at[h], far_in.at[h], f_send.at[h], f_recv.at[h], other_x, me_t)

    for q in (1, 0):
        for h in range(CHUNKS):
            for r in (1, 2, 3):
                rcopy(term_out.at[q, r, h], term_in.at[q, tok_of(r), h], e_send.at[q, r, h], e_recv.at[q, r, h], me_v, tok_of(r)).wait_recv()
            for k in range(depth - 1, 0, -1):
                @pl.when(z + k < depth)
                def _():
                    zz = z + k

                    @pl.when(z > 0)
                    def _():
                        eu_copy(q, zz, h).wait_recv()
                        up_out[q, zz, h] = (
                            term_in[q, zz, h].astype(F32) + up_in[q, zz, h].astype(F32)
                        ).astype(BF)

                    @pl.when(z == 0)
                    def _():
                        up_out[q, zz, h] = term_in[q, zz, h]

                    eu_copy(q, zz, h).start()

                @pl.when(z - k >= 0)
                def _():
                    zz = z - k

                    @pl.when(z < depth - 1)
                    def _():
                        ed_copy(q, zz, h).wait_recv()
                        down_out[q, zz, h] = (
                            term_in[q, zz, h].astype(F32) + down_in[q, zz, h].astype(F32)
                        ).astype(BF)

                    @pl.when(z == depth - 1)
                    def _():
                        down_out[q, zz, h] = term_in[q, zz, h]

                    ed_copy(q, zz, h).start()

    for q in (1, 0):
        for h in range(CHUNKS):
            @pl.when(z > 0)
            def _():
                eu_copy(q, z, h).wait_recv()

            @pl.when(z < depth - 1)
            def _():
                ed_copy(q, z, h).wait_recv()

            def total():
                own = term_in[q, z, h].astype(F32)
                below = jnp.where(z > 0, up_in[q, z, h].astype(F32), 0.0)
                above = jnp.where(z < depth - 1, down_in[q, z, h].astype(F32), 0.0)
                return own + below + above

            if q == 1:
                far_out[h] = total().astype(BF)
                far_copy(h).start()
            else:
                far_copy(h).wait_recv()
                out_ref[span(h), :] = (total() + far_in[h].astype(F32)).astype(BF)

    for h in range(CHUNKS):
        x_copy(h).wait_send()
        far_copy(h).wait_send()
        for q in range(2):
            for s in range(depth):
                @pl.when(z - s >= 0)
                def _():
                    @pl.when(z < depth - 1)
                    def _():
                        up_copy(q, z - s, h).wait_send()

                @pl.when(z + s < depth)
                def _():
                    @pl.when(z > 0)
                    def _():
                        down_copy(q, z + s, h).wait_send()

                @pl.when(me_t != s)
                def _():
                    t_copy(q, s, h).wait_send()

            for k in range(1, depth):
                @pl.when(z + k < depth)
                def _():
                    eu_copy(q, z + k, h).wait_send()

                @pl.when(z - k >= 0)
                def _():
                    ed_copy(q, z - k, h).wait_send()

            for r in range(1, 4):
                term_copy(q, r, h).wait_send()
    for k in range(2):
        pair_copy(k).wait_send()
    cross_copy().wait_send()
    for k in range(1, nv):
        stat_copy(k).wait_send()
    for i in range(3):
        grad_copy(i).wait_send()


def fused(vocab_size, tok_size):
    depth = vocab_size // 2

    def on_device(hidden, head_weight, targets, vocab_mask, token_grad):
        rows, feats = hidden.shape
        width = head_weight.shape[1]
        part = rows // CHUNKS
        dma = pltpu.SemaphoreType.DMA
        block = (CHUNKS, part, feats)
        by_q = (2, depth, CHUNKS)
        vmem = pl.BlockSpec(memory_space=pltpu.VMEM)
        hidden_grad, loss = pl.pallas_call(
            lambda *refs: kernel(depth, *refs),
            out_shape=(
                jax.ShapeDtypeStruct((rows, feats), BF),
                jax.ShapeDtypeStruct((8, 256), F32),
            ),
            in_specs=[pl.BlockSpec(memory_space=pltpu.HBM)] + [vmem] * 4,
            out_specs=(vmem, vmem),
            scratch_shapes=[
                pltpu.VMEM((2, depth) + block, BF),
                pltpu.VMEM((2, 4) + block, BF),
                pltpu.VMEM((4, rows, width), F32),
                pltpu.VMEM((2, rows, width), F32),
                pltpu.VMEM((rows, width), F32),
                pltpu.VMEM((rows, width), F32),
                pltpu.VMEM((4, rows, width), BF),
                pltpu.VMEM((8, 256), F32),
                pltpu.VMEM((vocab_size, 8, 256), F32),
                pltpu.VMEM((2, 4) + block, BF),
                pltpu.VMEM((2, 4) + block, BF),
                pltpu.VMEM((2, depth) + block, BF),
                pltpu.VMEM((2, depth) + block, BF),
                pltpu.VMEM((2, depth) + block, BF),
                pltpu.VMEM((2, depth) + block, BF),
                pltpu.VMEM(block, BF),
                pltpu.VMEM(block, BF),
                dma((CHUNKS,)), dma((CHUNKS,)), dma((CHUNKS,)),
                dma(by_q), dma(by_q), dma(by_q), dma(by_q), dma(by_q), dma(by_q),
                dma((2,)), dma((2,)), dma((1,)), dma((1,)),
                dma((vocab_size,)), dma((vocab_size,)), dma((3,)), dma((3,)),
                dma(by_q), dma(by_q), dma(by_q), dma(by_q), dma(by_q), dma(by_q),
                dma((CHUNKS,)), dma((CHUNKS,)),
            ],
            compiler_params=pltpu.CompilerParams(
                collective_id=0, has_side_effects=True, vmem_limit_bytes=60 * 1024 * 1024
            ),
        )(hidden, head_weight, targets[:, None], vocab_mask[None, :], token_grad[:, None])
        return (hidden_grad, loss[0, :rows])

    return on_device


def solution(mesh):
    placed = (P("tok", "vocab"), P("tok", "vocab"), P("tok"), P("vocab"), P("tok"))
    vocab_size, tok_size = mesh.shape["vocab"], mesh.shape["tok"]

    def body(hidden, *rest):
        fits = tok_size == 4 and vocab_size == 2 * tok_size and hidden.shape[1] % 128 == 0
        build = fused if fits and hidden.shape[0] <= 256 else make_on_device
        return build(vocab_size, tok_size)(hidden, *rest)

    return jax.shard_map(
        body,
        mesh=mesh,
        in_specs=placed,
        out_specs=(P("tok", "vocab"), P("tok")),
        check_vma=False,
    )
```

```python
import jax
import jax.numpy as jnp
from jax import lax
from jax.experimental import pallas as pl
from jax.experimental.pallas import tpu as pltpu
from jax.sharding import PartitionSpec as P


def make_on_device(vocab_size, tok_size):
    share = vocab_size // tok_size
    moves = [
        (b * tok_size + a, (a * share + b % share) * tok_size + b // share)
        for a in range(tok_size)
        for b in range(vocab_size)
    ]
    back = [(there, here) for here, there in moves]

    def on_device(hidden, head_weight, targets, vocab_mask, token_grad):
        rows, feats = hidden.shape
        block_width = head_weight.shape[1]
        moved = lax.ppermute(hidden, ("vocab", "tok"), moves)
        pieces = lax.all_gather(moved, "vocab")
        gathered = (
            pieces.reshape(tok_size, share, rows, feats)
            .transpose(0, 2, 1, 3)
            .reshape(tok_size * rows, share * feats)
        )
        partial_logits = jnp.dot(gathered, head_weight, preferred_element_type=jnp.float32)
        logits = lax.psum_scatter(partial_logits, "tok", scatter_dimension=0, tiled=True)
        first_column = lax.axis_index("vocab") * block_width
        masked = jnp.where(vocab_mask[None, :] == 1, logits, jnp.float32(-1e30))
        local_max = jnp.max(masked, axis=1)
        columns = first_column + jnp.arange(block_width, dtype=jnp.int32)
        onehot = columns[None, :] == targets[:, None]
        local_target = jnp.sum(jnp.where(onehot, logits, jnp.float32(0.0)), axis=1)
        weights = jnp.exp(masked - local_max[:, None])
        local_sum = jnp.sum(weights, axis=1)
        stats = lax.all_gather(jnp.stack([local_max, local_sum, local_target]), "vocab")
        row_max = jnp.max(stats[:, 0], axis=0)
        denominator = jnp.sum(stats[:, 1] * jnp.exp(stats[:, 0] - row_max[None]), axis=0)
        target_logit = jnp.sum(stats[:, 2], axis=0)
        log_norm = row_max + jnp.log(denominator)
        token_loss = log_norm - target_logit
        probabilities = jnp.exp(masked - log_norm[:, None])
        logit_grad = (
            token_grad[:, None] * (probabilities - onehot.astype(jnp.float32))
        ).astype(jnp.bfloat16)
        all_grads = lax.all_gather(logit_grad, "tok", axis=0, tiled=True)
        partial_value = lax.dot_general(
            all_grads,
            head_weight,
            (((1,), (1,)), ((), ())),
            preferred_element_type=jnp.float32,
        )
        blocks = (
            partial_value.reshape(tok_size, rows, share, feats)
            .transpose(0, 2, 1, 3)
            .reshape(vocab_size, rows, feats)
        )
        summed = lax.psum_scatter(blocks, "vocab", scatter_dimension=0, tiled=False)
        hidden_grad = lax.ppermute(summed.astype(jnp.bfloat16), ("vocab", "tok"), back)
        return (hidden_grad, token_loss)

    return on_device


CHUNKS = 3
LATE = (0, 1)
EARLY = (2,)
ORDER = LATE + EARLY
BF = jnp.bfloat16
F32 = jnp.float32


def kernel(
    depth,
    hidden_ref, weight_ref, targets_ref, mask_ref, grad_ref,
    out_ref, loss_ref,
    gath, hb, plog, pair_in, cross_in, cross_out, dl, stats_out, stats_in,
    term_out, term_in, up_in, down_in, up_out, down_out, far_out, far_in, near, mix_out, mix_in,
    load_sem, x_send, x_recv, zu_send, zu_recv, zd_send, zd_recv, t_send, t_recv,
    p_send, p_recv, c_send, c_recv, s_send, s_recv, g_send, g_recv,
    e_send, e_recv, eu_send, eu_recv, ed_send, ed_recv, f_send, f_recv, w_send, w_recv, m_send, m_recv,
):
    rows, feats = hidden_ref.shape
    part = rows // CHUNKS
    width = weight_ref.shape[1]
    me_v = lax.axis_index("vocab")
    me_t = lax.axis_index("tok")
    z, x = me_v // 2, me_v % 2
    y, c = me_t // 2, me_t % 2
    nv = 2 * depth

    def dev(v, t):
        return {"vocab": v, "tok": t}

    def tok_of(r):
        return ((y + r // 2) % 2) * 2 + (c + r % 2) % 2

    other_x = z * 2 + (1 - x)

    def rcopy(src, dst, ss, rs, v, t):
        return pltpu.make_async_remote_copy(
            src_ref=src, dst_ref=dst, send_sem=ss, recv_sem=rs,
            device_id=dev(v, t), device_id_type=pl.DeviceIdType.MESH,
        )

    def span(h):
        return pl.ds(h * part, part)

    loads = [
        pltpu.make_async_copy(hidden_ref.at[span(h)], gath.at[0, z, h], load_sem.at[h])
        for h in range(CHUNKS)
    ]
    for load in loads:
        load.start()

    barrier = pltpu.get_barrier_semaphore()
    for r in range(1, 4):
        pl.semaphore_signal(barrier, inc=1, device_id=dev(me_v, tok_of(r)), device_id_type=pl.DeviceIdType.MESH)
    for k in range(1, nv):
        pl.semaphore_signal(barrier, inc=1, device_id=dev((me_v + k) % nv, me_t), device_id_type=pl.DeviceIdType.MESH)
    pl.semaphore_wait(barrier, 3 + nv - 1)

    top = jnp.concatenate([targets_ref[...].astype(F32), grad_ref[...]], axis=0)
    top = jnp.concatenate([top, jnp.zeros((2, 256 - rows), F32)], axis=1)
    sides = jnp.transpose(jnp.concatenate([top, jnp.zeros((126, 256), F32)], axis=0))[0:rows]
    tok_target = sides[:, 0:1].astype(jnp.int32)
    tok_grad = sides[:, 1:2]

    def x_copy(h):
        return rcopy(gath.at[0, z, h], gath.at[1, z, h], x_send.at[h], x_recv.at[h], other_x, me_t)

    def up_copy(q, zz, h):
        return rcopy(gath.at[q, zz, h], gath.at[q, zz, h], zu_send.at[q, zz, h], zu_recv.at[q, zz, h], me_v + 2, me_t)

    def down_copy(q, zz, h):
        return rcopy(gath.at[q, zz, h], gath.at[q, zz, h], zd_send.at[q, zz, h], zd_recv.at[q, zz, h], me_v - 2, me_t)

    def rel(zz):
        return 2 * ((zz // 2 + y) % 2) + (zz % 2 + c) % 2

    def t_copy(q, zz, h):
        r = rel(zz)
        return rcopy(gath.at[q, zz, h], hb.at[q, r, h], t_send.at[q, zz, h], t_recv.at[q, r, h], me_v, zz)

    def pass_on(q, zz, h):
        @pl.when(zz != me_t)
        def _():
            t_copy(q, zz, h).start()

    def late_x(r, h):
        source = gath.at[0, me_t, h] if r == 0 else hb.at[0, r, h]
        return rcopy(source, hb.at[1, r, h], w_send.at[r, h], w_recv.at[r, h], other_x, me_t)

    def await_own(r, h):
        rcopy(gath.at[0, 0, h], hb.at[0, r, h], t_send.at[0, 0, h], t_recv.at[0, r, h], me_v, tok_of(1)).wait_recv()

    def late_others():
        for h in LATE:
            for r in range(1, 4):
                await_own(r, h)
                late_x(r, h).start()

    distance = jnp.where(z > me_t, z - me_t, me_t - z)
    for h in range(CHUNKS):
        loads[h].wait()
    for h in EARLY:
        x_copy(h).start()
    for s in range(depth):
        for h in ORDER:
            for q in range(1 if h in LATE else 2):
                if s == 0:
                    if q == 1:
                        x_copy(h).wait_recv()

                    @pl.when(z < depth - 1)
                    def _():
                        up_copy(q, z, h).start()

                    @pl.when(z > 0)
                    def _():
                        down_copy(q, z, h).start()

                    pass_on(q, z, h)
                else:
                    @pl.when(z - s >= 0)
                    def _():
                        up_copy(q, z - s, h).wait_recv()

                        @pl.when(z < depth - 1)
                        def _():
                            up_copy(q, z - s, h).start()

                        pass_on(q, z - s, h)

                    @pl.when(z + s < depth)
                    def _():
                        down_copy(q, z + s, h).wait_recv()

                        @pl.when(z > 0)
                        def _():
                            down_copy(q, z + s, h).start()

                        pass_on(q, z + s, h)

        @pl.when(distance == s)
        def _():
            for h in LATE:
                late_x(0, h).start()

        if s > 0:
            @pl.when(distance == s - 1)
            def _():
                late_others()

    @pl.when(distance == depth - 1)
    def _():
        late_others()

    for h in range(CHUNKS):
        hb[0, 0, h] = gath[0, me_t, h]
    for h in EARLY:
        hb[1, 0, h] = gath[1, me_t, h]

    def weight_rows(q):
        owner = (x + q) % 2
        return pl.ds(pl.multiple_of(owner * feats, 128), feats)

    tile = 256

    def logits_of(r0, nr):
        @pl.loop(0, width // tile)
        def _(j):
            cols = pl.ds(pl.multiple_of(j * tile, tile), tile)
            total = None
            for q in range(2):
                lhs = hb[q, pl.ds(r0, nr)].reshape(nr * rows, feats)
                term = jnp.dot(lhs, weight_ref[weight_rows(q), cols], preferred_element_type=F32)
                total = term if total is None else total + term
            plog[pl.ds(r0, nr), :, cols] = total.reshape(nr, rows, tile)

    def pair_copy(k):
        return rcopy(plog.at[1 + 2 * k], pair_in.at[k], p_send.at[k], p_recv.at[k], me_v, tok_of(1))

    def cross_copy():
        return rcopy(cross_out, cross_in, c_send.at[0], c_recv.at[0], me_v, tok_of(2))

    def await_rel(r):
        for h in EARLY:
            if r > 0:
                for q in range(2):
                    rcopy(gath.at[q, 0, h], hb.at[q, r, h], t_send.at[q, 0, h], t_recv.at[q, r, h], me_v, tok_of(1)).wait_recv()
        for h in LATE:
            late_x(r, h).wait_recv()

    await_rel(2)
    await_rel(3)
    logits_of(2, 2)
    pair_copy(1).start()
    await_rel(1)
    await_rel(0)
    logits_of(0, 2)
    pair_copy(0).start()
    pair_copy(1).wait_recv()
    cross_out[...] = plog[2] + pair_in[1]
    cross_copy().start()
    pair_copy(0).wait_recv()
    plog[0] = plog[0] + pair_in[0]
    cross_copy().wait_recv()
    logits = plog[0] + cross_in[...]

    masked = jnp.where(mask_ref[...] == 1, logits, jnp.float32(-1e30))
    local_max = jnp.max(masked, axis=1, keepdims=True)
    columns = me_v * width + lax.broadcasted_iota(jnp.int32, (rows, width), 1)
    onehot = columns == tok_target
    local_target = jnp.sum(jnp.where(onehot, logits, 0.0), axis=1, keepdims=True)
    local_sum = jnp.sum(jnp.exp(masked - local_max), axis=1, keepdims=True)
    lanes = lax.broadcasted_iota(jnp.int32, (rows, 128), 1)
    packed = jnp.where(lanes == 0, local_max, jnp.where(lanes == 1, local_sum, local_target))
    tall = jnp.concatenate([packed, jnp.zeros((256 - rows, 128), F32)], axis=0)
    mine = jnp.transpose(tall)[0:8]
    stats_out[...] = mine
    stats_in[me_v] = mine
    plog[0] = masked

    def stat_copy(k):
        return rcopy(stats_out, stats_in.at[me_v], s_send.at[k], s_recv.at[me_v], (me_v + k) % nv, me_t)

    for k in range(1, nv):
        stat_copy(k).start()
    for k in range(1, nv):
        source = (me_v + nv - k) % nv
        rcopy(stats_out, stats_in.at[source], s_send.at[k], s_recv.at[source], source, me_t).wait_recv()
    row_max = stats_in[0][0:1]
    for v in range(1, nv):
        row_max = jnp.maximum(row_max, stats_in[v][0:1])
    denominator = jnp.zeros_like(row_max)
    target_logit = jnp.zeros_like(row_max)
    for v in range(nv):
        got = stats_in[v]
        denominator += got[1:2] * jnp.exp(got[0:1] - row_max)
        target_logit += got[2:3]
    log_norm = row_max + jnp.log(denominator)
    loss_ref[...] = (log_norm - target_logit)[:, 0:rows]
    column = jnp.transpose(jnp.broadcast_to(log_norm, (128, 256)))[0:rows, 0:1]
    probabilities = jnp.exp(plog[0] - column)
    dl[0] = (tok_grad * (probabilities - onehot.astype(F32))).astype(BF)

    def grad_copy(i):
        if i == 0:
            return rcopy(dl.at[0], dl.at[2], g_send.at[0], g_recv.at[0], me_v, tok_of(2))
        if i == 1:
            return rcopy(dl.at[0], dl.at[1], g_send.at[1], g_recv.at[1], me_v, tok_of(1))
        return rcopy(dl.at[2], dl.at[3], g_send.at[2], g_recv.at[2], me_v, tok_of(1))

    grad_copy(0).start()
    grad_copy(1).start()

    def term_copy(q, r, h):
        return rcopy(
            term_out.at[q, r, h], term_in.at[q, me_t, h], e_send.at[q, r, h], e_recv.at[q, r, h], me_v, tok_of(r)
        )

    def mix_copy(r, h):
        return rcopy(mix_out.at[r, h], mix_in.at[r, h], m_send.at[r, h], m_recv.at[r, h], other_x, me_t)

    def terms_of(q, r0, nr):
        lhs = dl[pl.ds(r0, nr)].reshape(nr * rows, width)
        value = lax.dot_general(
            lhs, weight_ref[weight_rows(q), :], (((1,), (1,)), ((), ())), preferred_element_type=F32
        ).reshape(nr, CHUNKS, part, feats)
        for i in range(nr):
            r = r0 + i
            for h in EARLY:
                if r == 0:
                    term_in[q, me_t, h] = value[i, h].astype(BF)
                else:
                    term_out[q, r, h] = value[i, h].astype(BF)
                    term_copy(q, r, h).start()
            for h in LATE:
                if q == 0:
                    near[r, h] = value[i, h]
                else:
                    mix_out[r, h] = value[i, h].astype(BF)
                    mix_copy(r, h).start()

    grad_copy(1).wait_recv()
    for q in (1, 0):
        terms_of(q, 0, 2)
    grad_copy(0).wait_recv()
    grad_copy(2).start()
    for q in (1, 0):
        terms_of(q, 2, 1)
    grad_copy(2).wait_recv()
    for q in (1, 0):
        terms_of(q, 3, 1)
    for r in range(4):
        for h in LATE:
            mix_copy(r, h).wait_recv()
            both = (near[r, h] + mix_in[r, h].astype(F32)).astype(BF)
            if r == 0:
                term_in[0, me_t, h] = both
            else:
                term_out[0, r, h] = both
                term_copy(0, r, h).start()

    def eu_copy(q, zz, h):
        return rcopy(up_out.at[q, zz, h], up_in.at[q, zz, h], eu_send.at[q, zz, h], eu_recv.at[q, zz, h], me_v + 2, me_t)

    def ed_copy(q, zz, h):
        return rcopy(down_out.at[q, zz, h], down_in.at[q, zz, h], ed_send.at[q, zz, h], ed_recv.at[q, zz, h], me_v - 2, me_t)

    def far_copy(h):
        return rcopy(far_out.at[h], far_in.at[h], f_send.at[h], f_recv.at[h], other_x, me_t)

    streams = [(q, h) for h in EARLY for q in (1, 0)] + [(0, h) for h in LATE]
    for q, h in streams:
        if True:
            for r in (1, 2, 3):
                rcopy(term_out.at[q, r, h], term_in.at[q, tok_of(r), h], e_send.at[q, r, h], e_recv.at[q, r, h], me_v, tok_of(r)).wait_recv()
            for k in range(depth - 1, 0, -1):
                @pl.when(z + k < depth)
                def _():
                    zz = z + k

                    @pl.when(z > 0)
                    def _():
                        eu_copy(q, zz, h).wait_recv()
                        up_out[q, zz, h] = (
                            term_in[q, zz, h].astype(F32) + up_in[q, zz, h].astype(F32)
                        ).astype(BF)

                    @pl.when(z == 0)
                    def _():
                        up_out[q, zz, h] = term_in[q, zz, h]

                    eu_copy(q, zz, h).start()

                @pl.when(z - k >= 0)
                def _():
                    zz = z - k

                    @pl.when(z < depth - 1)
                    def _():
                        ed_copy(q, zz, h).wait_recv()
                        down_out[q, zz, h] = (
                            term_in[q, zz, h].astype(F32) + down_in[q, zz, h].astype(F32)
                        ).astype(BF)

                    @pl.when(z == depth - 1)
                    def _():
                        down_out[q, zz, h] = term_in[q, zz, h]

                    ed_copy(q, zz, h).start()

    for q, h in streams:
        if True:
            @pl.when(z > 0)
            def _():
                eu_copy(q, z, h).wait_recv()

            @pl.when(z < depth - 1)
            def _():
                ed_copy(q, z, h).wait_recv()

            def total():
                own = term_in[q, z, h].astype(F32)
                below = jnp.where(z > 0, up_in[q, z, h].astype(F32), 0.0)
                above = jnp.where(z < depth - 1, down_in[q, z, h].astype(F32), 0.0)
                return own + below + above

            if q == 1:
                far_out[h] = total().astype(BF)
                far_copy(h).start()
            elif h in LATE:
                out_ref[span(h), :] = total().astype(BF)
            else:
                far_copy(h).wait_recv()
                out_ref[span(h), :] = (total() + far_in[h].astype(F32)).astype(BF)

    for h in range(CHUNKS):
        if h in EARLY:
            x_copy(h).wait_send()
            far_copy(h).wait_send()
        else:
            for r in range(4):
                late_x(r, h).wait_send()
                mix_copy(r, h).wait_send()
        for q in range(1 if h in LATE else 2):
            for s in range(depth):
                @pl.when(z - s >= 0)
                def _():
                    @pl.when(z < depth - 1)
                    def _():
                        up_copy(q, z - s, h).wait_send()

                @pl.when(z + s < depth)
                def _():
                    @pl.when(z > 0)
                    def _():
                        down_copy(q, z + s, h).wait_send()

                @pl.when(me_t != s)
                def _():
                    t_copy(q, s, h).wait_send()

            for k in range(1, depth):
                @pl.when(z + k < depth)
                def _():
                    eu_copy(q, z + k, h).wait_send()

                @pl.when(z - k >= 0)
                def _():
                    ed_copy(q, z - k, h).wait_send()

            for r in range(1, 4):
                term_copy(q, r, h).wait_send()
    for k in range(2):
        pair_copy(k).wait_send()
    cross_copy().wait_send()
    for k in range(1, nv):
        stat_copy(k).wait_send()
    for i in range(3):
        grad_copy(i).wait_send()


def fused(vocab_size, tok_size):
    depth = vocab_size // 2

    def on_device(hidden, head_weight, targets, vocab_mask, token_grad):
        rows, feats = hidden.shape
        width = head_weight.shape[1]
        part = rows // CHUNKS
        dma = pltpu.SemaphoreType.DMA
        block = (CHUNKS, part, feats)
        by_q = (2, depth, CHUNKS)
        vmem = pl.BlockSpec(memory_space=pltpu.VMEM)
        hidden_grad, loss = pl.pallas_call(
            lambda *refs: kernel(depth, *refs),
            out_shape=(
                jax.ShapeDtypeStruct((rows, feats), BF),
                jax.ShapeDtypeStruct((1, rows), F32),
            ),
            in_specs=[pl.BlockSpec(memory_space=pltpu.HBM)] + [vmem] * 4,
            out_specs=(vmem, vmem),
            scratch_shapes=[
                pltpu.VMEM((2, depth) + block, BF),
                pltpu.VMEM((2, 4) + block, BF),
                pltpu.VMEM((4, rows, width), F32),
                pltpu.VMEM((2, rows, width), F32),
                pltpu.VMEM((rows, width), F32),
                pltpu.VMEM((rows, width), F32),
                pltpu.VMEM((4, rows, width), BF),
                pltpu.VMEM((8, 256), F32),
                pltpu.VMEM((vocab_size, 8, 256), F32),
                pltpu.VMEM((2, 4) + block, BF),
                pltpu.VMEM((2, 4) + block, BF),
                pltpu.VMEM((2, depth) + block, BF),
                pltpu.VMEM((2, depth) + block, BF),
                pltpu.VMEM((2, depth) + block, BF),
                pltpu.VMEM((2, depth) + block, BF),
                pltpu.VMEM(block, BF),
                pltpu.VMEM(block, BF),
                pltpu.VMEM((4,) + block, F32),
                pltpu.VMEM((4,) + block, BF),
                pltpu.VMEM((4,) + block, BF),
                dma((CHUNKS,)), dma((CHUNKS,)), dma((CHUNKS,)),
                dma(by_q), dma(by_q), dma(by_q), dma(by_q), dma(by_q), dma(by_q),
                dma((2,)), dma((2,)), dma((1,)), dma((1,)),
                dma((vocab_size,)), dma((vocab_size,)), dma((3,)), dma((3,)),
                dma(by_q), dma(by_q), dma(by_q), dma(by_q), dma(by_q), dma(by_q),
                dma((CHUNKS,)), dma((CHUNKS,)),
                dma((4, CHUNKS)), dma((4, CHUNKS)), dma((4, CHUNKS)), dma((4, CHUNKS)),
            ],
            compiler_params=pltpu.CompilerParams(
                collective_id=0, has_side_effects=True, vmem_limit_bytes=60 * 1024 * 1024
            ),
        )(hidden, head_weight, targets[None, :], vocab_mask[None, :], token_grad[None, :])
        return (hidden_grad, loss.reshape(rows))

    return on_device


def solution(mesh):
    placed = (P("tok", "vocab"), P("tok", "vocab"), P("tok"), P("vocab"), P("tok"))
    vocab_size, tok_size = mesh.shape["vocab"], mesh.shape["tok"]

    def body(hidden, *rest):
        fits = tok_size == 4 and vocab_size == 2 * tok_size and hidden.shape[1] % 128 == 0
        build = fused if fits and hidden.shape[0] <= 256 else make_on_device
        return build(vocab_size, tok_size)(hidden, *rest)

    return jax.shard_map(
        body,
        mesh=mesh,
        in_specs=placed,
        out_specs=(P("tok", "vocab"), P("tok")),
        check_vma=False,
    )
```

```python
import jax
import jax.numpy as jnp
from jax import lax
from jax.experimental import pallas as pl
from jax.experimental.pallas import tpu as pltpu
from jax.sharding import PartitionSpec as P


def make_on_device(vocab_size, tok_size):
    share = vocab_size // tok_size
    moves = [
        (b * tok_size + a, (a * share + b % share) * tok_size + b // share)
        for a in range(tok_size)
        for b in range(vocab_size)
    ]
    back = [(there, here) for here, there in moves]

    def on_device(hidden, head_weight, targets, vocab_mask, token_grad):
        rows, feats = hidden.shape
        block_width = head_weight.shape[1]
        moved = lax.ppermute(hidden, ("vocab", "tok"), moves)
        pieces = lax.all_gather(moved, "vocab")
        gathered = (
            pieces.reshape(tok_size, share, rows, feats)
            .transpose(0, 2, 1, 3)
            .reshape(tok_size * rows, share * feats)
        )
        partial_logits = jnp.dot(gathered, head_weight, preferred_element_type=jnp.float32)
        logits = lax.psum_scatter(partial_logits, "tok", scatter_dimension=0, tiled=True)
        first_column = lax.axis_index("vocab") * block_width
        masked = jnp.where(vocab_mask[None, :] == 1, logits, jnp.float32(-1e30))
        local_max = jnp.max(masked, axis=1)
        columns = first_column + jnp.arange(block_width, dtype=jnp.int32)
        onehot = columns[None, :] == targets[:, None]
        local_target = jnp.sum(jnp.where(onehot, logits, jnp.float32(0.0)), axis=1)
        weights = jnp.exp(masked - local_max[:, None])
        local_sum = jnp.sum(weights, axis=1)
        stats = lax.all_gather(jnp.stack([local_max, local_sum, local_target]), "vocab")
        row_max = jnp.max(stats[:, 0], axis=0)
        denominator = jnp.sum(stats[:, 1] * jnp.exp(stats[:, 0] - row_max[None]), axis=0)
        target_logit = jnp.sum(stats[:, 2], axis=0)
        log_norm = row_max + jnp.log(denominator)
        token_loss = log_norm - target_logit
        probabilities = jnp.exp(masked - log_norm[:, None])
        logit_grad = (
            token_grad[:, None] * (probabilities - onehot.astype(jnp.float32))
        ).astype(jnp.bfloat16)
        all_grads = lax.all_gather(logit_grad, "tok", axis=0, tiled=True)
        partial_value = lax.dot_general(
            all_grads,
            head_weight,
            (((1,), (1,)), ((), ())),
            preferred_element_type=jnp.float32,
        )
        blocks = (
            partial_value.reshape(tok_size, rows, share, feats)
            .transpose(0, 2, 1, 3)
            .reshape(vocab_size, rows, feats)
        )
        summed = lax.psum_scatter(blocks, "vocab", scatter_dimension=0, tiled=False)
        hidden_grad = lax.ppermute(summed.astype(jnp.bfloat16), ("vocab", "tok"), back)
        return (hidden_grad, token_loss)

    return on_device


CHUNKS = 3
LATE = (0, 1)
EARLY = (2,)
ORDER = LATE + EARLY
BF = jnp.bfloat16
F32 = jnp.float32


def kernel(
    depth,
    hidden_ref, weight_ref, targets_ref, mask_ref, grad_ref,
    out_ref, loss_ref,
    gath, hb, plog, pair_in, cross_in, cross_out, dl, stats_out, stats_in,
    term_out, term_in, up_in, down_in, up_out, down_out, far_out, far_in, near, mix_out, mix_in,
    load_sem, x_send, x_recv, zu_send, zu_recv, zd_send, zd_recv, t_send, t_recv,
    p_send, p_recv, c_send, c_recv, s_send, s_recv, g_send, g_recv,
    e_send, e_recv, eu_send, eu_recv, ed_send, ed_recv, f_send, f_recv, w_send, w_recv, m_send, m_recv,
):
    rows, feats = hidden_ref.shape
    part = rows // CHUNKS
    width = weight_ref.shape[1]
    me_v = lax.axis_index("vocab")
    me_t = lax.axis_index("tok")
    z, x = me_v // 2, me_v % 2
    y, c = me_t // 2, me_t % 2
    nv = 2 * depth

    def dev(v, t):
        return {"vocab": v, "tok": t}

    def tok_of(r):
        return ((y + r // 2) % 2) * 2 + (c + r % 2) % 2

    other_x = z * 2 + (1 - x)

    def rcopy(src, dst, ss, rs, v, t):
        return pltpu.make_async_remote_copy(
            src_ref=src, dst_ref=dst, send_sem=ss, recv_sem=rs,
            device_id=dev(v, t), device_id_type=pl.DeviceIdType.MESH,
        )

    def span(h):
        return pl.ds(h * part, part)

    loads = [
        pltpu.make_async_copy(hidden_ref.at[span(h)], gath.at[0, z, h], load_sem.at[h])
        for h in range(CHUNKS)
    ]
    for load in loads:
        load.start()

    barrier = pltpu.get_barrier_semaphore()
    for r in range(1, 4):
        pl.semaphore_signal(barrier, inc=1, device_id=dev(me_v, tok_of(r)), device_id_type=pl.DeviceIdType.MESH)
    for k in range(1, nv):
        pl.semaphore_signal(barrier, inc=1, device_id=dev((me_v + k) % nv, me_t), device_id_type=pl.DeviceIdType.MESH)
    pl.semaphore_wait(barrier, 3 + nv - 1)

    top = jnp.concatenate([targets_ref[...].astype(F32), grad_ref[...]], axis=0)
    top = jnp.concatenate([top, jnp.zeros((2, 256 - rows), F32)], axis=1)
    sides = jnp.transpose(jnp.concatenate([top, jnp.zeros((126, 256), F32)], axis=0))[0:rows]
    tok_target = sides[:, 0:1].astype(jnp.int32)
    tok_grad = sides[:, 1:2]

    def x_copy(h):
        return rcopy(gath.at[0, z, h], gath.at[1, z, h], x_send.at[h], x_recv.at[h], other_x, me_t)

    def up_copy(q, zz, h):
        return rcopy(gath.at[q, zz, h], gath.at[q, zz, h], zu_send.at[q, zz, h], zu_recv.at[q, zz, h], me_v + 2, me_t)

    def down_copy(q, zz, h):
        return rcopy(gath.at[q, zz, h], gath.at[q, zz, h], zd_send.at[q, zz, h], zd_recv.at[q, zz, h], me_v - 2, me_t)

    def rel(zz):
        return 2 * ((zz // 2 + y) % 2) + (zz % 2 + c) % 2

    def t_copy(q, zz, h):
        r = rel(zz)
        return rcopy(gath.at[q, zz, h], hb.at[q, r, h], t_send.at[q, zz, h], t_recv.at[q, r, h], me_v, zz)

    def pass_on(q, zz, h):
        @pl.when(zz != me_t)
        def _():
            t_copy(q, zz, h).start()

    def late_x(r, h):
        source = gath.at[0, me_t, h] if r == 0 else hb.at[0, r, h]
        return rcopy(source, hb.at[1, r, h], w_send.at[r, h], w_recv.at[r, h], other_x, me_t)

    def await_own(r, h):
        rcopy(gath.at[0, 0, h], hb.at[0, r, h], t_send.at[0, 0, h], t_recv.at[0, r, h], me_v, tok_of(1)).wait_recv()

    def late_others():
        for h in LATE:
            for r in range(1, 4):
                await_own(r, h)
                late_x(r, h).start()

    distance = jnp.where(z > me_t, z - me_t, me_t - z)
    for h in range(CHUNKS):
        loads[h].wait()
    for h in EARLY:
        x_copy(h).start()
    for s in range(depth):
        for h in ORDER:
            if h == EARLY[0]:
                @pl.when(distance == s)
                def _():
                    for late in LATE:
                        late_x(0, late).start()

                if s > 0:
                    @pl.when(distance == s - 1)
                    def _():
                        late_others()

                if s == depth - 1:
                    @pl.when(distance == s)
                    def _():
                        late_others()

            for q in range(1 if h in LATE else 2):
                if s == 0:
                    if q == 1:
                        x_copy(h).wait_recv()

                    @pl.when(z < depth - 1)
                    def _():
                        up_copy(q, z, h).start()

                    @pl.when(z > 0)
                    def _():
                        down_copy(q, z, h).start()

                    pass_on(q, z, h)
                else:
                    @pl.when(z - s >= 0)
                    def _():
                        up_copy(q, z - s, h).wait_recv()

                        @pl.when(z < depth - 1)
                        def _():
                            up_copy(q, z - s, h).start()

                        pass_on(q, z - s, h)

                    @pl.when(z + s < depth)
                    def _():
                        down_copy(q, z + s, h).wait_recv()

                        @pl.when(z > 0)
                        def _():
                            down_copy(q, z + s, h).start()

                        pass_on(q, z + s, h)

    for h in range(CHUNKS):
        hb[0, 0, h] = gath[0, me_t, h]
    for h in EARLY:
        hb[1, 0, h] = gath[1, me_t, h]

    def weight_rows(q):
        owner = (x + q) % 2
        return pl.ds(pl.multiple_of(owner * feats, 128), feats)

    tile = 256

    def logits_of(r0, nr, group):
        c0, nc = len(LATE) * group, len((LATE, EARLY)[group])

        @pl.loop(0, width // tile)
        def _(j):
            cols = pl.ds(pl.multiple_of(j * tile, tile), tile)
            total = None
            for q in range(2):
                lhs = hb[q, pl.ds(r0, nr), pl.ds(c0, nc)].reshape(nr * nc * part, feats)
                term = jnp.dot(lhs, weight_ref[weight_rows(q), cols], preferred_element_type=F32)
                total = term if total is None else total + term
            plog[pl.ds(r0, nr), pl.ds(c0 * part, nc * part), cols] = total.reshape(nr, nc * part, tile)

    def group_rows(group):
        return pl.ds(part * len(LATE) * group, part * len((LATE, EARLY)[group]))

    def pair_copy(k, group):
        return rcopy(
            plog.at[1 + 2 * k, group_rows(group)], pair_in.at[k, group_rows(group)],
            p_send.at[k, group], p_recv.at[k, group], me_v, tok_of(1),
        )

    def cross_copy(group):
        return rcopy(
            cross_out.at[group_rows(group)], cross_in.at[group_rows(group)],
            c_send.at[group], c_recv.at[group], me_v, tok_of(2),
        )

    def cross_over(group):
        pair_copy(1, group).wait_recv()
        cross_out[group_rows(group), :] = plog[2, group_rows(group), :] + pair_in[1, group_rows(group), :]
        cross_copy(group).start()

    for r in range(1, 4):
        for h in EARLY:
            for q in range(2):
                rcopy(gath.at[q, 0, h], hb.at[q, r, h], t_send.at[q, 0, h], t_recv.at[q, r, h], me_v, tok_of(1)).wait_recv()
    logits_of(0, 4, 1)
    pair_copy(1, 1).start()
    pair_copy(0, 1).start()
    cross_over(1)
    for r in (2, 3):
        for h in LATE:
            late_x(r, h).wait_recv()
    logits_of(2, 2, 0)
    pair_copy(1, 0).start()
    cross_over(0)
    for r in (0, 1):
        for h in LATE:
            late_x(r, h).wait_recv()
    logits_of(0, 2, 0)
    pair_copy(0, 0).start()
    for group in (1, 0):
        pair_copy(0, group).wait_recv()
    plog[0] = plog[0] + pair_in[0]
    for group in (1, 0):
        cross_copy(group).wait_recv()
    logits = plog[0] + cross_in[...]

    masked = jnp.where(mask_ref[...] == 1, logits, jnp.float32(-1e30))
    local_max = jnp.max(masked, axis=1, keepdims=True)
    columns = me_v * width + lax.broadcasted_iota(jnp.int32, (rows, width), 1)
    onehot = columns == tok_target
    local_target = jnp.sum(jnp.where(onehot, logits, 0.0), axis=1, keepdims=True)
    local_sum = jnp.sum(jnp.exp(masked - local_max), axis=1, keepdims=True)
    lanes = lax.broadcasted_iota(jnp.int32, (rows, 128), 1)
    packed = jnp.where(lanes == 0, local_max, jnp.where(lanes == 1, local_sum, local_target))
    tall = jnp.concatenate([packed, jnp.zeros((256 - rows, 128), F32)], axis=0)
    mine = jnp.transpose(tall)[0:8]
    stats_out[...] = mine
    stats_in[me_v] = mine
    plog[0] = masked

    def stat_copy(k):
        return rcopy(stats_out, stats_in.at[me_v], s_send.at[k], s_recv.at[me_v], (me_v + k) % nv, me_t)

    for k in range(1, nv):
        stat_copy(k).start()
    for k in range(1, nv):
        source = (me_v + nv - k) % nv
        rcopy(stats_out, stats_in.at[source], s_send.at[k], s_recv.at[source], source, me_t).wait_recv()
    row_max = stats_in[0][0:1]
    for v in range(1, nv):
        row_max = jnp.maximum(row_max, stats_in[v][0:1])
    denominator = jnp.zeros_like(row_max)
    target_logit = jnp.zeros_like(row_max)
    for v in range(nv):
        got = stats_in[v]
        denominator += got[1:2] * jnp.exp(got[0:1] - row_max)
        target_logit += got[2:3]
    log_norm = row_max + jnp.log(denominator)
    loss_ref[...] = (log_norm - target_logit)[:, 0:rows]
    column = jnp.transpose(jnp.broadcast_to(log_norm, (128, 256)))[0:rows, 0:1]
    probabilities = jnp.exp(plog[0] - column)
    dl[0] = (tok_grad * (probabilities - onehot.astype(F32))).astype(BF)

    def grad_copy(i):
        if i == 0:
            return rcopy(dl.at[0], dl.at[2], g_send.at[0], g_recv.at[0], me_v, tok_of(2))
        if i == 1:
            return rcopy(dl.at[0], dl.at[1], g_send.at[1], g_recv.at[1], me_v, tok_of(1))
        return rcopy(dl.at[2], dl.at[3], g_send.at[2], g_recv.at[2], me_v, tok_of(1))

    grad_copy(0).start()
    grad_copy(1).start()

    def term_copy(q, r, h):
        return rcopy(
            term_out.at[q, r, h], term_in.at[q, me_t, h], e_send.at[q, r, h], e_recv.at[q, r, h], me_v, tok_of(r)
        )

    def mix_copy(r, h):
        return rcopy(mix_out.at[r, h], mix_in.at[r, h], m_send.at[r, h], m_recv.at[r, h], other_x, me_t)

    def terms_of(q, r0, nr):
        lhs = dl[pl.ds(r0, nr)].reshape(nr * rows, width)
        value = lax.dot_general(
            lhs, weight_ref[weight_rows(q), :], (((1,), (1,)), ((), ())), preferred_element_type=F32
        ).reshape(nr, CHUNKS, part, feats)
        for i in range(nr):
            r = r0 + i
            for h in EARLY:
                if r == 0:
                    term_in[q, me_t, h] = value[i, h].astype(BF)
                else:
                    term_out[q, r, h] = value[i, h].astype(BF)
                    term_copy(q, r, h).start()
            for h in LATE:
                if q == 0:
                    near[r, h] = value[i, h]
                else:
                    mix_out[r, h] = value[i, h].astype(BF)
                    mix_copy(r, h).start()

    grad_copy(1).wait_recv()
    for q in (1, 0):
        terms_of(q, 0, 2)
    grad_copy(0).wait_recv()
    grad_copy(2).start()
    for q in (1, 0):
        terms_of(q, 2, 1)
    grad_copy(2).wait_recv()
    for q in (1, 0):
        terms_of(q, 3, 1)
    for r in range(4):
        for h in LATE:
            mix_copy(r, h).wait_recv()
            both = (near[r, h] + mix_in[r, h].astype(F32)).astype(BF)
            if r == 0:
                term_in[0, me_t, h] = both
            else:
                term_out[0, r, h] = both
                term_copy(0, r, h).start()

    def eu_copy(q, zz, h):
        return rcopy(up_out.at[q, zz, h], up_in.at[q, zz, h], eu_send.at[q, zz, h], eu_recv.at[q, zz, h], me_v + 2, me_t)

    def ed_copy(q, zz, h):
        return rcopy(down_out.at[q, zz, h], down_in.at[q, zz, h], ed_send.at[q, zz, h], ed_recv.at[q, zz, h], me_v - 2, me_t)

    def far_copy(h):
        return rcopy(far_out.at[h], far_in.at[h], f_send.at[h], f_recv.at[h], other_x, me_t)

    streams = [(q, h) for h in EARLY for q in (1, 0)] + [(0, h) for h in LATE]
    for q, h in streams:
        if True:
            for r in (1, 2, 3):
                rcopy(term_out.at[q, r, h], term_in.at[q, tok_of(r), h], e_send.at[q, r, h], e_recv.at[q, r, h], me_v, tok_of(r)).wait_recv()
            for k in range(depth - 1, 0, -1):
                @pl.when(z + k < depth)
                def _():
                    zz = z + k

                    @pl.when(z > 0)
                    def _():
                        eu_copy(q, zz, h).wait_recv()
                        up_out[q, zz, h] = (
                            term_in[q, zz, h].astype(F32) + up_in[q, zz, h].astype(F32)
                        ).astype(BF)

                    @pl.when(z == 0)
                    def _():
                        up_out[q, zz, h] = term_in[q, zz, h]

                    eu_copy(q, zz, h).start()

                @pl.when(z - k >= 0)
                def _():
                    zz = z - k

                    @pl.when(z < depth - 1)
                    def _():
                        ed_copy(q, zz, h).wait_recv()
                        down_out[q, zz, h] = (
                            term_in[q, zz, h].astype(F32) + down_in[q, zz, h].astype(F32)
                        ).astype(BF)

                    @pl.when(z == depth - 1)
                    def _():
                        down_out[q, zz, h] = term_in[q, zz, h]

                    ed_copy(q, zz, h).start()

    for q, h in streams:
        if True:
            @pl.when(z > 0)
            def _():
                eu_copy(q, z, h).wait_recv()

            @pl.when(z < depth - 1)
            def _():
                ed_copy(q, z, h).wait_recv()

            def total():
                own = term_in[q, z, h].astype(F32)
                below = jnp.where(z > 0, up_in[q, z, h].astype(F32), 0.0)
                above = jnp.where(z < depth - 1, down_in[q, z, h].astype(F32), 0.0)
                return own + below + above

            if q == 1:
                far_out[h] = total().astype(BF)
                far_copy(h).start()
            elif h in LATE:
                out_ref[span(h), :] = total().astype(BF)
            else:
                far_copy(h).wait_recv()
                out_ref[span(h), :] = (total() + far_in[h].astype(F32)).astype(BF)

    for h in range(CHUNKS):
        if h in EARLY:
            x_copy(h).wait_send()
            far_copy(h).wait_send()
        else:
            for r in range(4):
                late_x(r, h).wait_send()
                mix_copy(r, h).wait_send()
        for q in range(1 if h in LATE else 2):
            for s in range(depth):
                @pl.when(z - s >= 0)
                def _():
                    @pl.when(z < depth - 1)
                    def _():
                        up_copy(q, z - s, h).wait_send()

                @pl.when(z + s < depth)
                def _():
                    @pl.when(z > 0)
                    def _():
                        down_copy(q, z + s, h).wait_send()

                @pl.when(me_t != s)
                def _():
                    t_copy(q, s, h).wait_send()

            for k in range(1, depth):
                @pl.when(z + k < depth)
                def _():
                    eu_copy(q, z + k, h).wait_send()

                @pl.when(z - k >= 0)
                def _():
                    ed_copy(q, z - k, h).wait_send()

            for r in range(1, 4):
                term_copy(q, r, h).wait_send()
    for group in range(2):
        for k in range(2):
            pair_copy(k, group).wait_send()
        cross_copy(group).wait_send()
    for k in range(1, nv):
        stat_copy(k).wait_send()
    for i in range(3):
        grad_copy(i).wait_send()


def fused(vocab_size, tok_size):
    depth = vocab_size // 2

    def on_device(hidden, head_weight, targets, vocab_mask, token_grad):
        rows, feats = hidden.shape
        width = head_weight.shape[1]
        part = rows // CHUNKS
        dma = pltpu.SemaphoreType.DMA
        block = (CHUNKS, part, feats)
        by_q = (2, depth, CHUNKS)
        vmem = pl.BlockSpec(memory_space=pltpu.VMEM)
        hidden_grad, loss = pl.pallas_call(
            lambda *refs: kernel(depth, *refs),
            out_shape=(
                jax.ShapeDtypeStruct((rows, feats), BF),
                jax.ShapeDtypeStruct((1, rows), F32),
            ),
            in_specs=[pl.BlockSpec(memory_space=pltpu.HBM)] + [vmem] * 4,
            out_specs=(vmem, vmem),
            scratch_shapes=[
                pltpu.VMEM((2, depth) + block, BF),
                pltpu.VMEM((2, 4) + block, BF),
                pltpu.VMEM((4, rows, width), F32),
                pltpu.VMEM((2, rows, width), F32),
                pltpu.VMEM((rows, width), F32),
                pltpu.VMEM((rows, width), F32),
                pltpu.VMEM((4, rows, width), BF),
                pltpu.VMEM((8, 256), F32),
                pltpu.VMEM((vocab_size, 8, 256), F32),
                pltpu.VMEM((2, 4) + block, BF),
                pltpu.VMEM((2, 4) + block, BF),
                pltpu.VMEM((2, depth) + block, BF),
                pltpu.VMEM((2, depth) + block, BF),
                pltpu.VMEM((2, depth) + block, BF),
                pltpu.VMEM((2, depth) + block, BF),
                pltpu.VMEM(block, BF),
                pltpu.VMEM(block, BF),
                pltpu.VMEM((4,) + block, F32),
                pltpu.VMEM((4,) + block, BF),
                pltpu.VMEM((4,) + block, BF),
                dma((CHUNKS,)), dma((CHUNKS,)), dma((CHUNKS,)),
                dma(by_q), dma(by_q), dma(by_q), dma(by_q), dma(by_q), dma(by_q),
                dma((2, 2)), dma((2, 2)), dma((2,)), dma((2,)),
                dma((vocab_size,)), dma((vocab_size,)), dma((3,)), dma((3,)),
                dma(by_q), dma(by_q), dma(by_q), dma(by_q), dma(by_q), dma(by_q),
                dma((CHUNKS,)), dma((CHUNKS,)),
                dma((4, CHUNKS)), dma((4, CHUNKS)), dma((4, CHUNKS)), dma((4, CHUNKS)),
            ],
            compiler_params=pltpu.CompilerParams(
                collective_id=0, has_side_effects=True, vmem_limit_bytes=60 * 1024 * 1024
            ),
        )(hidden, head_weight, targets[None, :], vocab_mask[None, :], token_grad[None, :])
        return (hidden_grad, loss.reshape(rows))

    return on_device


def solution(mesh):
    placed = (P("tok", "vocab"), P("tok", "vocab"), P("tok"), P("vocab"), P("tok"))
    vocab_size, tok_size = mesh.shape["vocab"], mesh.shape["tok"]

    def body(hidden, *rest):
        fits = tok_size == 4 and vocab_size == 2 * tok_size and hidden.shape[1] % 128 == 0
        build = fused if fits and hidden.shape[0] <= 256 else make_on_device
        return build(vocab_size, tok_size)(hidden, *rest)

    return jax.shard_map(
        body,
        mesh=mesh,
        in_specs=placed,
        out_specs=(P("tok", "vocab"), P("tok")),
        check_vma=False,
    )
```
